32 devices in a mesh: dp: 1 (over z), ei: 4 (over y), eo: 8 (over x, core).
Axes of the slice: x: 4, y: 4, z: 1, core: 2. Of those that a mesh axis runs over, the one named last changes fastest.
The devices are a block of a 4x4x8 slice.
Arguments:
- tokens: bfloat16 [6144, 2048], P(('dp', 'ei', 'eo'))
- expert_idx: int32 [6144, 8], P(('dp', 'ei', 'eo'))
- gates: float32 [6144, 8], P(('dp', 'ei', 'eo'))
- w_gate: bfloat16 [32, 2048, 1024], P(('ei', 'eo'))
- w_up: bfloat16 [32, 2048, 1024], P(('ei', 'eo'))
- w_down: bfloat16 [32, 1024, 2048], P(('ei', 'eo'))
- grad_out: bfloat16 [6144, 2048], P(('dp', 'ei', 'eo'))
Outputs:
- output 1: bfloat16 [6144, 2048], P(('dp', 'ei', 'eo'))
- output 2: bfloat16 [6144, 2048], P(('dp', 'ei', 'eo'))
- output 3: float32 [6144, 8], P(('dp', 'ei', 'eo'))
- output 4: bfloat16 [32, 2048, 1024], P(('dp', 'ei', 'eo'))
- output 5: bfloat16 [32, 2048, 1024], P(('dp', 'ei', 'eo'))
- output 6: bfloat16 [32, 1024, 2048], P(('dp', 'ei', 'eo'))
All inputs are finite; a program needn't handle non-finite values.
Results may differ from the reference program's by a relative error of at most 0.00784686.
Values are sent between devices in bfloat16 or wider.
A program may use at most 768 MiB of HBM per device.

```python
import jax
import jax.numpy as jnp
from jax import lax

GROUP_DEVS = 32
EXP_DEV = 1
TOK_DEV = 192
D_MODEL = 2048
D_FF = 1024
TOP_K = 8
NUM_EXPERTS = EXP_DEV * GROUP_DEVS
TOKENS = TOK_DEV * GROUP_DEVS
CAPACITY = min(TOK_DEV, TOK_DEV * TOP_K // (4 * EXP_DEV))


def draw_routes(route_key):
    hot_key, src_key = jax.random.split(route_key)
    hot_dev = jax.random.randint(hot_key, (), 0, GROUP_DEVS)
    expert_ids = jnp.arange(NUM_EXPERTS, dtype=jnp.int32)
    is_hot = expert_ids // EXP_DEV == hot_dev
    cold_n = NUM_EXPERTS - EXP_DEV
    rest_n = TOK_DEV * TOP_K - EXP_DEV * CAPACITY
    above_hot = (expert_ids >= (hot_dev + 1) * EXP_DEV).astype(jnp.int32)
    cold_pos = jnp.clip(expert_ids - EXP_DEV * above_hot, 0, cold_n - 1)
    positions = jnp.arange(TOK_DEV * TOP_K, dtype=jnp.int32)

    def one_source(source_key):
        perm_key, row_key, rot_key = jax.random.split(source_key, 3)
        cold_rank = jax.random.permutation(perm_key, cold_n)
        cold_count = rest_n // cold_n + (cold_rank[cold_pos] < rest_n % cold_n).astype(jnp.int32)
        counts = jnp.where(is_hot, CAPACITY, cold_count).astype(jnp.int32)
        listing = jnp.searchsorted(jnp.cumsum(counts), positions, side='right').astype(jnp.int32)
        route_table = listing.reshape(TOP_K, TOK_DEV).T[jax.random.permutation(row_key, TOK_DEV)]
        row_shift = jax.random.randint(rot_key, (TOK_DEV, 1), 0, TOP_K)
        col_order = (jnp.arange(TOP_K)[None, :] + row_shift) % TOP_K
        return jnp.take_along_axis(route_table, col_order, axis=1)

    source_keys = jax.random.split(src_key, GROUP_DEVS)
    return jax.vmap(one_source)(source_keys).reshape(TOKENS, TOP_K).astype(jnp.int32)


def setup_inputs(seed: int = 0, part: int = 0) -> dict:
    part_key = jax.random.fold_in(jax.random.key(seed), part)
    tok_key, route_key, gate_key, dy_key = jax.random.split(part_key, 4)
    gate_w_key, up_w_key, down_w_key = jax.random.split(jax.random.key(seed + 1), 3)
    tokens = jax.random.normal(tok_key, (TOKENS, D_MODEL), jnp.float32).astype(jnp.bfloat16)
    expert_idx = draw_routes(route_key)
    gates = jax.random.uniform(gate_key, (TOKENS, TOP_K), jnp.float32, 0.05, 0.3)
    w_gate = (jax.random.normal(gate_w_key, (NUM_EXPERTS, D_MODEL, D_FF), jnp.float32) * D_MODEL ** -0.5).astype(jnp.bfloat16)
    w_up = (jax.random.normal(up_w_key, (NUM_EXPERTS, D_MODEL, D_FF), jnp.float32) * D_MODEL ** -0.5).astype(jnp.bfloat16)
    w_down = (jax.random.normal(down_w_key, (NUM_EXPERTS, D_FF, D_MODEL), jnp.float32) * D_FF ** -0.5).astype(jnp.bfloat16)
    grad_out = jax.random.normal(dy_key, (TOKENS, D_MODEL), jnp.float32).astype(jnp.bfloat16)
    return {'tokens': tokens, 'expert_idx': expert_idx, 'gates': gates, 'w_gate': w_gate, 'w_up': w_up, 'w_down': w_down, 'grad_out': grad_out}


def reference(tokens, expert_idx, gates, w_gate, w_up, w_down, grad_out):
    n_assign = TOKENS * TOP_K
    expert_cap = GROUP_DEVS * CAPACITY
    flat_e = expert_idx.reshape(-1)
    sort_order = jnp.argsort(flat_e, stable=True).astype(jnp.int32)
    sorted_e = flat_e[sort_order]
    counts = jnp.zeros((NUM_EXPERTS,), jnp.int32).at[flat_e].add(1)
    starts = jnp.cumsum(counts) - counts
    slot_rank = jnp.arange(n_assign, dtype=jnp.int32) - starts[sorted_e]
    filler = jnp.full((NUM_EXPERTS * expert_cap,), n_assign, jnp.int32).at[sorted_e * expert_cap + slot_rank].set(sort_order)
    filler = filler.reshape(NUM_EXPERTS, expert_cap)
    tok_pad = jnp.concatenate([tokens, jnp.zeros((1, D_MODEL), tokens.dtype)])
    dy_pad = jnp.concatenate([grad_out, jnp.zeros((1, D_MODEL), grad_out.dtype)])
    gate_pad = jnp.concatenate([gates.reshape(-1), jnp.zeros((1,), jnp.float32)])

    def one_expert(acc_state, expert_in):
        out_acc, dx_acc, dg_acc = acc_state
        wg_e, wu_e, wd_e, assign = expert_in
        tok_ids = assign // TOP_K
        x_rows = tok_pad[tok_ids]
        g_rows = gate_pad[assign]
        dy_rows = dy_pad[tok_ids]
        h_gate = jnp.dot(x_rows, wg_e, preferred_element_type=jnp.float32)
        h_up = jnp.dot(x_rows, wu_e, preferred_element_type=jnp.float32)
        sig_gate = jax.nn.sigmoid(h_gate)
        hidden = (h_gate * sig_gate * h_up).astype(jnp.bfloat16)
        y_rows = jnp.dot(hidden, wd_e, preferred_element_type=jnp.float32).astype(jnp.bfloat16)
        dg_rows = jnp.sum(dy_rows.astype(jnp.float32) * y_rows.astype(jnp.float32), axis=1)
        u_rows = (g_rows[:, None] * dy_rows.astype(jnp.float32)).astype(jnp.bfloat16)
        d_hidden = jnp.dot(u_rows, wd_e.T, preferred_element_type=jnp.float32)
        d_up = (d_hidden * h_gate * sig_gate).astype(jnp.bfloat16)
        d_gate = (d_hidden * h_up * sig_gate * (1.0 + h_gate * (1.0 - sig_gate))).astype(jnp.bfloat16)
        dx_rows = (jnp.dot(d_gate, wg_e.T, preferred_element_type=jnp.float32) + jnp.dot(d_up, wu_e.T, preferred_element_type=jnp.float32)).astype(jnp.bfloat16)
        dw_gate = jnp.dot(x_rows.T, d_gate, preferred_element_type=jnp.float32).astype(jnp.bfloat16)
        dw_up = jnp.dot(x_rows.T, d_up, preferred_element_type=jnp.float32).astype(jnp.bfloat16)
        dw_down = jnp.dot(hidden.T, u_rows, preferred_element_type=jnp.float32).astype(jnp.bfloat16)
        out_acc = out_acc.at[tok_ids].add(g_rows[:, None] * y_rows.astype(jnp.float32))
        dx_acc = dx_acc.at[tok_ids].add(dx_rows.astype(jnp.float32))
        dg_acc = dg_acc.at[assign].add(dg_rows)
        return (out_acc, dx_acc, dg_acc), (dw_gate, dw_up, dw_down)

    zero_state = (jnp.zeros((TOKENS + 1, D_MODEL), jnp.float32), jnp.zeros((TOKENS + 1, D_MODEL), jnp.float32), jnp.zeros((n_assign + 1,), jnp.float32))
    final_state, weight_grads = lax.scan(one_expert, zero_state, (w_gate, w_up, w_down, filler))
    out_acc, dx_acc, dg_acc = final_state
    dw_gate, dw_up, dw_down = weight_grads
    layer_out = out_acc[:TOKENS].astype(jnp.bfloat16)
    grad_tokens = dx_acc[:TOKENS].astype(jnp.bfloat16)
    grad_gates = dg_acc[:n_assign].reshape(TOKENS, TOP_K)
    return (layer_out, grad_tokens, grad_gates, dw_gate, dw_up, dw_down)
```

```python
import jax
import jax.numpy as jnp
from jax import lax
from jax.sharding import PartitionSpec as P

GROUP = ('ei', 'eo')


def solution(mesh):
    eo_size = mesh.shape['eo']
    tok_spec = P(('dp', 'ei', 'eo'))
    exp_spec = P(('ei', 'eo'))
    f32, bf16 = jnp.float32, jnp.bfloat16

    def dot(x, y, dims):
        return lax.dot_general(x, y, (dims, ((), ())), preferred_element_type=f32)

    def device_step(tok_loc, idx_loc, gate_loc, w_gate, w_up, w_down, dy_loc):
        tok_dev = tok_loc.shape[0]
        me = lax.axis_index('ei') * eo_size + lax.axis_index('eo')
        wg, wu, wd = w_gate[0], w_up[0], w_down[0]
        x = lax.all_gather(tok_loc, GROUP, axis=0, tiled=True)
        ids = lax.all_gather(idx_loc, GROUP, axis=0, tiled=True)
        gates = lax.all_gather(gate_loc, GROUP, axis=0, tiled=True)
        dy = lax.all_gather(dy_loc, GROUP, axis=0, tiled=True)
        hit = ids == me
        mask = jnp.any(hit, axis=1)[:, None]
        gate = jnp.sum(jnp.where(hit, gates, 0.0), axis=1)[:, None]
        a = dot(x, wg, ((1,), (0,)))
        b = dot(x, wu, ((1,), (0,)))
        s = jax.nn.sigmoid(a)
        h = jnp.where(mask, a * s * b, 0.0).astype(bf16)
        o = dot(h, wd, ((1,), (0,))).astype(bf16)
        y = lax.psum_scatter(gate * o.astype(f32), GROUP, scatter_dimension=0, tiled=True).astype(bf16)
        dyf = dy.astype(f32)
        dgate = jnp.sum(dyf * o.astype(f32), axis=1).reshape(-1, tok_dev)
        dgate = lax.all_gather(dgate[None], GROUP, axis=0, tiled=True)[:, me]
        dgate = jnp.take_along_axis(dgate.T, idx_loc, axis=1)
        u = (gate * dyf).astype(bf16)
        q = dot(u, wd, ((1,), (1,)))
        du = jnp.where(mask, q * a * s, 0.0).astype(bf16)
        dg = jnp.where(mask, q * b * s * (1.0 + a * (1.0 - s)), 0.0).astype(bf16)
        dx = (dot(dg, wg, ((1,), (1,))) + dot(du, wu, ((1,), (1,)))).astype(bf16)
        dx = lax.psum_scatter(dx.astype(f32), GROUP, scatter_dimension=0, tiled=True).astype(bf16)
        dwg = dot(x, dg, ((0,), (0,))).astype(bf16)[None]
        dwu = dot(x, du, ((0,), (0,))).astype(bf16)[None]
        dwd = dot(h, u, ((0,), (0,))).astype(bf16)[None]
        return y, dx, dgate, dwg, dwu, dwd

    return jax.shard_map(device_step, mesh=mesh, in_specs=(tok_spec, tok_spec, tok_spec, exp_spec, exp_spec, exp_spec, tok_spec), out_specs=(tok_spec,) * 6, check_vma=False)
```

```python
import functools
import jax
import jax.numpy as jnp
from jax import lax
from jax.experimental import pallas as pl
from jax.experimental.pallas import tpu as pltpu
from jax.sharding import PartitionSpec as P

LANES, SUBLANES = 128, 8
MESH = pl.DeviceIdType.MESH
RING = 4
BACK = RING - 1
KK = (0, 1)
HOPS = ((0, 1), (0, -1), (1, 1), (1, -1))
NEIGHBOURS = ((1, 0), (BACK, 0), (0, 1), (0, BACK))
ANY = pl.BlockSpec(memory_space=pl.ANY)
f32, bf16 = jnp.float32, jnp.bfloat16
VMEM_LIMIT = 62 * 1024 * 1024


class Place:
    def __init__(self, tok_dev, half):
        self.dp, self.y, eo = lax.axis_index('dp'), lax.axis_index('ei'), lax.axis_index('eo')
        self.x, self.c = eo // 2, eo % 2
        self.tok_dev, self.half = tok_dev, half

    def chip(self, r1, r2, c=None):
        c = self.c if c is None else c
        dx, dy = (1 - c) * r1 + c * r2, (1 - c) * r2 + c * r1
        return (self.y + dy) % RING, (self.x + dx) % RING

    def device(self, r1, r2):
        y, x = self.chip(r1, r2)
        return (self.dp, y, 2 * x + self.c)

    def partner(self):
        return (self.dp, self.y, 2 * self.x + 1 - self.c)

    def rows(self, r1, r2, kk, c=None):
        c = self.c if c is None else c
        y, x = self.chip(r1, r2, c)
        return pl.ds(pl.multiple_of(((y * RING + x) * 2 + (c + kk) % 2) * self.tok_dev, self.tok_dev), self.tok_dev)

    def cols(self, mine=True):
        return pl.ds(pl.multiple_of((self.c if mine else 1 - self.c) * self.half, self.half), self.half)

    def greet(self):
        barrier = pltpu.get_barrier_semaphore()
        peers = [self.partner()] + [self.device(*r) for r in NEIGHBOURS]
        for peer in peers:
            pl.semaphore_signal(barrier, inc=1, device_id=peer, device_id_type=MESH)
        pl.semaphore_wait(barrier, len(peers))


def hops(r):
    return min(r, RING - r)


def ag_order():
    chips = sorted(((r1, r2) for r1 in range(RING) for r2 in range(RING)), key=lambda r: (hops(r[0]) + hops(r[1]), r[1]))[1:]
    near = len(NEIGHBOURS)
    return [(*r, kk) for kk in KK for r in chips[:near]] + [(*r, kk) for r in chips[near:] for kk in KK]


class Gather:
    N_SEMS = 5

    def __init__(self, place, loc, out, send, recv, d2d_send, d2d_recv, misc):
        self.p, self.loc, self.out = place, loc, out
        self.send, self.recv, self.d2d_send, self.d2d_recv, self.misc = send, recv, d2d_send, d2d_recv, misc

    @staticmethod
    def scratch():
        s = pltpu.SemaphoreType.DMA
        return [s((2, 2, RING, RING, 2)), s((RING, RING, 2)), s((RING, RING, 2)), s((RING, RING, 2)), s((3,))]

    def piece(self, r1, r2, kk):
        return self.out.at[self.p.rows(r1, r2, kk), self.p.cols()]

    def hop(self, axis, step, r1, r2, kk, src=None):
        to = (step % RING, 0) if axis == 0 else (0, step % RING)
        t1, t2 = (r1 - to[0]) % RING, (r2 - to[1]) % RING
        dst = self.piece(r1, r2, kk)
        return pltpu.make_async_remote_copy(
            src_ref=dst if src is None else src, dst_ref=dst, send_sem=self.send.at[axis, (1 - step) // 2, r1, r2, kk],
            recv_sem=self.recv.at[t1, t2, kk], device_id=self.p.device(*to), device_id_type=MESH)

    def arrived(self, r1, r2, kk):
        ref = self.piece(r1, r2, kk)
        pltpu.make_async_copy(ref, ref, self.recv.at[r1, r2, kk]).wait()

    def d2d(self, r1, r2, kk):
        ref = self.piece(r1, r2, kk)
        return pltpu.make_async_remote_copy(src_ref=ref, dst_ref=ref, send_sem=self.d2d_send.at[r1, r2, kk],
                                            recv_sem=self.d2d_recv.at[r1, r2, kk], device_id=self.p.partner(), device_id_type=MESH)

    def own(self):
        p = self.p
        rows = p.rows(0, 0, 0)
        local = pltpu.make_async_copy(self.loc, self.out.at[rows], self.misc.at[0])
        swap = pltpu.make_async_remote_copy(src_ref=self.loc, dst_ref=self.out.at[rows], send_sem=self.misc.at[1],
                                            recv_sem=self.misc.at[2], device_id=p.partner(), device_id_type=MESH)
        return local, swap

    def begin(self):
        local, swap = self.own()
        swap.start()
        src = self.loc.at[:, self.p.cols()]
        for axis, step in HOPS:
            self.hop(axis, step, 0, 0, 0, src).start()
        local.start()

    def begin_partner(self):
        ref = self.out.at[self.p.rows(0, 0, 1)]
        pltpu.make_async_copy(ref, ref, self.misc.at[2]).wait()
        for axis, step in HOPS:
            self.hop(axis, step, 0, 0, 1).start()

    def sends_of(self, r1, r2, kk):
        if r1 == r2 == 0:
            return HOPS
        onward = [h for h, r, k in zip(HOPS[::2] + HOPS[1::2], (r1, r2) * 2, (0, 0, 1, 1)) if (r, k) == (BACK if k == 0 else 1, kk)]
        if r2 == 0:
            return [h for h in onward if h[0] == 0] + list(HOPS[2:])
        return [h for h in onward if h[0] == 1]

    def relay(self, r1, r2, kk):
        self.arrived(r1, r2, kk)
        for axis, step in self.sends_of(r1, r2, kk):
            self.hop(axis, step, r1, r2, kk).start()
        self.d2d(r1, r2, kk).start()

    def finish(self):
        local, swap = self.own()
        local.wait()
        swap.wait_send()
        src = self.loc.at[:, self.p.cols()]
        for kk in KK:
            for axis, step in self.sends_of(0, 0, kk):
                self.hop(axis, step, 0, 0, kk, src if kk == 0 else None).wait_send()
        for r1, r2, kk in ag_order():
            for axis, step in self.sends_of(r1, r2, kk):
                self.hop(axis, step, r1, r2, kk).wait_send()
            self.d2d(r1, r2, kk).wait_send()
            ref = self.out.at[self.p.rows(r1, r2, kk, 1 - self.p.c), self.p.cols(False)]
            pltpu.make_async_copy(ref, ref, self.d2d_recv.at[r1, r2, kk]).wait()


def ag_kernel(loc, table, out, table_out, *sems):
    gs = [Gather(Place(r.shape[0], r.shape[1] // 2), r, o, *sems[k * Gather.N_SEMS:(k + 1) * Gather.N_SEMS])
          for k, (r, o) in enumerate(((table, table_out), (loc, out)))]
    gs[0].p.greet()
    for g in gs:
        g.begin()
    for g in gs:
        g.begin_partner()
    for piece in ag_order():
        for g in gs:
            g.relay(*piece)
    for g in gs:
        g.finish()


def all_gather_rows(loc, table, group, cid):
    return pl.pallas_call(
        ag_kernel, out_shape=[jax.ShapeDtypeStruct((group * r.shape[0], r.shape[1]), r.dtype) for r in (loc, table)],
        in_specs=[ANY] * 2, out_specs=[ANY] * 2, scratch_shapes=Gather.scratch() * 2,
        compiler_params=pltpu.CompilerParams(collective_id=cid, has_side_effects=True), name='gather_rows')(loc, table)


LEGS = {'far': lambda d: (2, d, 0), 'near': lambda d: (1 + 2 * d, 1 - d, 2 - d), 'pass': lambda d: (1 + 2 * d, d, 1 + d)}


def rs_group(kind, r=None):
    ops = []
    arrived = lambda q, kk: [(q, d, 1 + kk) for d in KK]
    for d in KK:
        if kind == 'final':
            ops.append(dict(chip=(0, 0), kk=d, recvs=arrived(0, d) + arrived(RING, d), axis=None))
            continue
        off, kk, slot = LEGS[kind](d)
        q = RING if r is None else r
        recvs = [(q, d, 0)] if kind == 'pass' else []
        if r is None:
            ops.append(dict(chip=(off, 0), kk=kk, recvs=arrived(off, kk) + recvs, axis=0, step=1 - 2 * d, dst=(q, d, slot)))
        else:
            ops.append(dict(chip=(r, off), kk=kk, recvs=recvs, axis=1, step=1 - 2 * d, dst=(q, d, slot)))
    return ops


def rs_groups():
    order = [('far', 2), ('near', 2), ('far', 1), ('pass', 2), ('near', 1), ('far', BACK), ('pass', 1), ('near', BACK), ('far', 0), ('pass', BACK),
             ('far',), ('near', 0), ('pass', 0), ('near',), ('pass',), ('final',)]
    return [rs_group(*k) for k in order]


SLOTS = 8


class Scatter:
    def __init__(self, place, own, po, rbuf, out, gates, scratch):
        self.p, self.own, self.po, self.rbuf, self.out, self.gates = place, own, po, rbuf, out, gates
        (self.slots, self.in_o, self.in_p, self.in_r, self.fin, self.send, self.recv, self.d2d_send, self.d2d_recv, self.load,
         self.fin_sem) = scratch
        self.groups = rs_groups()
        self.n = 0
        for grp in self.groups:
            for op in grp:
                if op['axis'] is not None:
                    op['n'] = self.n
                    self.n += 1
        self.by_n = {op['n']: op for grp in self.groups for op in grp if op['axis'] is not None}

    @staticmethod
    def scratch(tok, half):
        s = pltpu.SemaphoreType.DMA
        return [pltpu.VMEM((SLOTS, tok, half), f32), pltpu.VMEM((2, tok, half), bf16), pltpu.VMEM((2, tok, half), bf16),
                pltpu.VMEM((2, 4, tok, half), f32), pltpu.VMEM((2, tok, half), bf16),
                s((30,)), s((RING + 1, 2, 3)), s((RING, RING, 2)), s((RING, RING, 2)), s((2, 6)), s((3,))]

    @staticmethod
    def hbm(tok, half, group):
        return [jax.ShapeDtypeStruct((group * tok, half), bf16), jax.ShapeDtypeStruct((RING + 1, 2, 3, tok, half), f32)]

    def swap(self, op):
        k = (*op['chip'], op['kk'])
        rows = self.p.rows(*k, 1 - self.p.c)
        return pltpu.make_async_remote_copy(
            src_ref=self.own.at[rows, self.p.cols(False)], dst_ref=self.po.at[rows], send_sem=self.d2d_send.at[k],
            recv_sem=self.d2d_recv.at[k], device_id=self.p.partner(), device_id_type=MESH)

    def begin(self):
        for grp in self.groups:
            for op in grp:
                self.swap(op).start()

    def loads(self, j, op):
        rows = self.p.rows(*op['chip'], op['kk'])
        out = [pltpu.make_async_copy(self.own.at[rows, self.p.cols()], self.in_o.at[j], self.load.at[j, 0]),
               pltpu.make_async_copy(self.po.at[rows], self.in_p.at[j], self.load.at[j, 1])]
        for i, r in enumerate(op['recvs']):
            out.append(pltpu.make_async_copy(self.rbuf.at[r], self.in_r.at[j, i], self.load.at[j, 2 + i]))
        return out

    def prep(self, g):
        for j, op in enumerate(self.groups[g]):
            k = (*op['chip'], op['kk'])
            rows = self.p.rows(*k)
            pltpu.make_async_copy(self.po.at[rows], self.po.at[rows], self.d2d_recv.at[k]).wait()
            for r in op['recvs']:
                pltpu.make_async_copy(self.rbuf.at[r], self.rbuf.at[r], self.recv.at[r]).wait()
            for copy in self.loads(j, op):
                copy.start()

    def sender(self, op):
        to = (op['step'] % RING, 0) if op['axis'] == 0 else (0, op['step'] % RING)
        return pltpu.make_async_remote_copy(
            src_ref=self.slots.at[op['n'] % SLOTS], dst_ref=self.rbuf.at[op['dst']], send_sem=self.send.at[op['n']],
            recv_sem=self.recv.at[op['dst']], device_id=self.p.device(*to), device_id_type=MESH)

    def fire(self, g):
        tok = self.p.tok_dev
        step = 32
        for j, op in enumerate(self.groups[g]):
            for copy in self.loads(j, op):
                copy.wait()
            sent = op['axis'] is not None
            if sent and op['n'] >= SLOTS:
                self.sender(self.by_n[op['n'] - SLOTS]).wait_send()
            y, x = self.p.chip(*op['chip'])
            row0 = ((y * RING + x) * 2 + (self.p.c + op['kk']) % 2) * tok

            def body(i, _):
                rows = pl.ds(pl.multiple_of(i * step, step), step)
                v = self.in_o[j, rows].astype(f32)
                w = self.in_p[j, rows].astype(f32)
                if self.gates is not None:
                    at = pl.ds(pl.multiple_of(row0 + i * step, step), step)
                    v = v * self.gates[at, 0:1]
                    w = w * self.gates[at, 2:3]
                v = v + w
                for r in range(len(op['recvs'])):
                    v = v + self.in_r[j, r, rows]
                if sent:
                    self.slots[op['n'] % SLOTS, rows] = v
                else:
                    self.fin[j, rows] = v.astype(bf16)
                return 0
            lax.fori_loop(0, tok // step, body, 0)
            if sent:
                self.sender(op).start()

    def result(self):
        dst = self.out.at[:, self.p.cols()]
        local = pltpu.make_async_copy(self.fin.at[0], dst, self.fin_sem.at[0])
        swap = pltpu.make_async_remote_copy(src_ref=self.fin.at[1], dst_ref=dst, send_sem=self.fin_sem.at[1], recv_sem=self.fin_sem.at[2],
                                            device_id=self.p.partner(), device_id_type=MESH)
        return local, swap

    def finish(self):
        local, swap = self.result()
        local.start()
        swap.start()
        for n in range(max(0, self.n - SLOTS), self.n):
            self.sender(self.by_n[n]).wait_send()
        for grp in self.groups:
            for op in grp:
                self.swap(op).wait_send()
        local.wait()
        swap.wait_send()
        ref = self.out.at[:, self.p.cols(False)]
        pltpu.make_async_copy(ref, ref, self.fin_sem.at[2]).wait()

    def before(self, step, at):
        @pl.when(step == 0)
        def _():
            self.p.greet()
            self.begin()
            self.prep(0)
            self.fire(0)
        for g in range(1, len(self.groups)):
            pl.when(step == at[g])(functools.partial(self.prep, g))

    def after(self, step, at):
        for g in range(1, len(self.groups)):
            pl.when(step == at[g])(functools.partial(self.fire, g))
        pl.when(step == at[-1])(self.finish)


def mm(x, y, cx, cy):
    return lax.dot_general(x, y, (((cx,), (cy,)), ((), ())), preferred_element_type=f32)


def forward_kernel(at, x, gm, wg, wu, wd, dy_loc, a_out, b_out, h_out, o_out, dy_out, *sems):
    i = pl.program_id(0)
    place = Place(dy_loc.shape[0], dy_loc.shape[1] // 2)
    g = Gather(place, dy_loc, dy_out, *sems)

    @pl.when(i == 0)
    def _():
        place.greet()
        g.begin()
        g.begin_partner()
    pieces = ag_order()
    for s in sorted(set(at)):
        @pl.when(i == s)
        def _():
            for piece, t in zip(pieces, at):
                if t == s:
                    g.relay(*piece)
    mask = gm[:, 1:2] > 0.0
    ff = wg.shape[1]
    n = ff // 2
    for k in range(2):
        cs = slice(k * n, (k + 1) * n)
        a = mm(x[...], wg[:, cs], 1, 0)
        b = mm(x[...], wu[:, cs], 1, 0)
        a_out[:, cs] = a
        b_out[:, cs] = b
        h_out[:, cs] = jnp.where(mask, a * jax.nn.sigmoid(a) * b, 0.0).astype(bf16)
    o_out[...] = mm(h_out[...], wd[...], 1, 0).astype(bf16)

    @pl.when(i == pl.num_programs(0) - 1)
    def _():
        g.finish()


FWD_LAST, BWD_LAST, WTS_LAST = 19, 21, 15


def schedule(steps, last):
    n = len(rs_groups())
    return [0] + [g * last // (n - 3) for g in range(n - 2)] + [steps - 1]


def rows_spec(tile, width):
    return pl.BlockSpec((tile, width), lambda i: (i, 0))


def whole_spec(shape):
    return pl.BlockSpec(shape, lambda i: (0,) * len(shape), pipeline_mode=pl.Buffered(1))


def params(cid):
    return pltpu.CompilerParams(collective_id=cid, has_side_effects=True, vmem_limit_bytes=VMEM_LIMIT, dimension_semantics=('arbitrary',))


def forward(x, gm, wg, wu, wd, dy_loc, cid, tile=256):
    n_tok, d = x.shape
    ff = wg.shape[1]
    steps = n_tok // tile
    at = [1 + k * FWD_LAST // len(ag_order()) for k in range(len(ag_order()))]
    S = jax.ShapeDtypeStruct
    return pl.pallas_call(
        functools.partial(forward_kernel, at), grid=(steps,),
        out_shape=[S((n_tok, ff), f32), S((n_tok, ff), f32), S((n_tok, ff), bf16), S((n_tok, d), bf16), S((n_tok, d), bf16)],
        in_specs=[rows_spec(tile, d), rows_spec(tile, gm.shape[1]), whole_spec(wg.shape), whole_spec(wu.shape), whole_spec(wd.shape), ANY],
        out_specs=[rows_spec(tile, ff), rows_spec(tile, ff), rows_spec(tile, ff), rows_spec(tile, d), ANY],
        scratch_shapes=Gather.scratch(), compiler_params=params(cid), name='forward')(x, gm, wg, wu, wd, dy_loc)


def backward_kernel(at, dy, gm, a, b, o, wg, wu, wd, gates, o_any, dg_out, du_out, u_out, dx_out, dgate_out, y_out, po, rbuf, *scratch):
    i = pl.program_id(0)
    tok, half = y_out.shape[0], y_out.shape[1] // 2
    rs = Scatter(Place(tok, half), o_any, po, rbuf, y_out, gates, scratch)
    rs.before(i, at)
    mask = gm[:, 1:2] > 0.0
    dyf = dy[...].astype(f32)
    u_out[...] = (gm[:, 0:1] * dyf).astype(bf16)
    dgate_out[...] = jnp.sum(dyf * o[...].astype(f32), axis=1, keepdims=True)
    n = wg.shape[1] // 2
    for k in range(2):
        cs = slice(k * n, (k + 1) * n)
        q = mm(u_out[...], wd[cs, :], 1, 1)
        av, bv = a[:, cs], b[:, cs]
        s = jax.nn.sigmoid(av)
        qs = q * s
        du_out[:, cs] = jnp.where(mask, q * av * s, 0.0).astype(bf16)
        dg_out[:, cs] = jnp.where(mask, q * bv * s * (1.0 + av * (1.0 - s)), 0.0).astype(bf16)
    dx_out[...] = (mm(dg_out[...], wg[...], 1, 1) + mm(du_out[...], wu[...], 1, 1)).astype(bf16)
    rs.after(i, at)


def backward(dy, gm, a, b, o, wg, wu, wd, tok, cid, tile=256):
    n_tok, d = dy.shape
    ff = wg.shape[1]
    steps = n_tok // tile
    at = schedule(steps, BWD_LAST)
    S = jax.ShapeDtypeStruct
    hbm = Scatter.hbm(tok, d // 2, n_tok // tok)
    out = pl.pallas_call(
        functools.partial(backward_kernel, at), grid=(steps,),
        out_shape=[S((n_tok, ff), bf16), S((n_tok, ff), bf16), S((n_tok, d), bf16), S((n_tok, d), bf16), S((n_tok, 1), f32), S((tok, d), bf16)] + hbm,
        in_specs=[rows_spec(tile, d), rows_spec(tile, gm.shape[1]), rows_spec(tile, ff), rows_spec(tile, ff), rows_spec(tile, d),
                  whole_spec(wg.shape), whole_spec(wu.shape), whole_spec(wd.shape), whole_spec(gm.shape), ANY],
        out_specs=[rows_spec(tile, ff), rows_spec(tile, ff), rows_spec(tile, d), rows_spec(tile, d), rows_spec(tile, 1), ANY, ANY, ANY],
        scratch_shapes=Scatter.scratch(tok, d // 2), compiler_params=params(cid), name='backward')(dy, gm, a, b, o, wg, wu, wd, gm, o)
    return out[:6]


def weights_kernel(at, n_k, x, dg, du, h, u, dx_any, dgate, dwg, dwu, dwd, dxs_out, dgate_out, po, rbuf, acc, stage, out_sem, *scratch):
    i = pl.program_id(0)
    tok, half = dxs_out.shape[0], dxs_out.shape[1] // 2
    rs = Scatter(Place(tok, half), dx_any, po, rbuf, dxs_out, None, scratch[Gather.N_SEMS:])
    rs.before(i, at)
    small = Gather(Place(dgate.shape[0], dgate.shape[1] // 2), dgate, dgate_out, *scratch[:Gather.N_SEMS])
    pieces = ag_order()
    far = [hops(r1) + hops(r2) for r1, r2, _ in pieces]
    pl.when(i == 0)(small.begin)
    pl.when(i == 1)(small.begin_partner)
    for k in sorted(set(far)):
        @pl.when(i == (3 * n_k - 2) * k // max(far))
        def _():
            for piece, n in zip(pieces, far):
                if n == k:
                    small.relay(*piece)
    pl.when(i == 3 * n_k - 1)(small.finish)
    ff = dg.shape[1]
    m = 256

    def flush(w, dst):
        return pltpu.make_async_copy(stage, dst, out_sem)

    def flush_d(k):
        return pltpu.make_async_copy(stage.at[pl.ds(k * ff, ff)], dwd.at[:, pl.ds(k * ff, ff)], out_sem)

    kc = i % n_k

    @pl.when(kc == 0)
    def _():
        def zero(r, _):
            acc[pl.ds(pl.multiple_of(r * 64, 64), 64)] = jnp.zeros((64, acc.shape[1]), f32)
            return 0
        lax.fori_loop(0, acc.shape[0] // 64, zero, 0)

    def add(left, right, row0=0, cols=None):
        def tile(r, _):
            lc = pl.ds(pl.multiple_of(r * m, m), m)
            rows = pl.ds(pl.multiple_of(row0 + r * m, m), m)
            acc[rows] += mm(left[:, lc], right[...] if cols is None else right[:, cols], 0, 0)
            return 0
        lax.fori_loop(0, left.shape[1] // m, tile, 0)

    pl.when(i < n_k)(lambda: add(x, dg))
    pl.when((i >= n_k) & (i < 2 * n_k))(lambda: add(x, du))

    @pl.when(i >= 2 * n_k)
    def _():
        for k in range(2):
            add(h, u, k * ff, slice(k * ff, (k + 1) * ff))

    @pl.when(i == 2 * n_k - 1)
    def _():
        flush(0, dwg).wait()

    @pl.when(i == 3 * n_k - 1)
    def _():
        flush(1, dwu).wait()

    @pl.when(kc == n_k - 1)
    def _():
        def conv(r, _):
            rows = pl.ds(pl.multiple_of(r * 64, 64), 64)
            stage[rows] = acc[rows].astype(bf16)
            return 0
        lax.fori_loop(0, acc.shape[0] // 64, conv, 0)

    pl.when(i == n_k - 1)(lambda: flush(0, dwg).start())
    pl.when(i == 2 * n_k - 1)(lambda: flush(1, dwu).start())

    @pl.when(i == 3 * n_k - 1)
    def _():
        flush_d(0).start()
        flush_d(1).start()
    rs.after(i, at)

    @pl.when(i == 3 * n_k - 1)
    def _():
        flush_d(0).wait()
        flush_d(1).wait()


def weights(x, dg, du, h, u, dx, dgate, tok, cid, tile=1024):
    n_tok, d = x.shape
    ff = dg.shape[1]
    n_k = n_tok // tile
    steps = 3 * n_k
    last = n_k - 1
    at = schedule(steps, WTS_LAST)
    S = jax.ShapeDtypeStruct
    hbm = Scatter.hbm(tok, d // 2, n_tok // tok)
    spec = lambda width, index: pl.BlockSpec((tile, width), lambda i: (index(i), 0))
    out = pl.pallas_call(
        functools.partial(weights_kernel, at, n_k), grid=(steps,),
        out_shape=[S((d, ff), bf16), S((d, ff), bf16), S((ff, d), bf16), S((tok, d), bf16), S((n_tok // tok * dgate.shape[0], dgate.shape[1]), f32)] + hbm,
        in_specs=[spec(d, lambda i: jnp.where(i < n_k, i, jnp.minimum(i - n_k, last))), spec(ff, lambda i: jnp.minimum(i, last)),
                  spec(ff, lambda i: jnp.clip(i - n_k, 0, last)), spec(ff, lambda i: jnp.maximum(i - 2 * n_k, 0)),
                  spec(d, lambda i: jnp.maximum(i - 2 * n_k, 0)), ANY, ANY],
        out_specs=[ANY] * 7,
        scratch_shapes=[pltpu.VMEM((d, ff), f32), pltpu.VMEM((d, ff), bf16), pltpu.SemaphoreType.DMA] + Gather.scratch() + Scatter.scratch(tok, d // 2),
        compiler_params=params(cid), name='weights')(x, dg, du, h, u, dx, dgate)
    return out[:5]


def solution(mesh):
    eo_size = mesh.shape['eo']
    group = mesh.shape['ei'] * eo_size
    tok_spec = P(('dp', 'ei', 'eo'))
    exp_spec = P(('ei', 'eo'))

    def device_step(tok_loc, idx_loc, gate_loc, w_gate, w_up, w_down, dy_loc):
        tok_dev, top_k = idx_loc.shape
        me = lax.axis_index('ei') * eo_size + lax.axis_index('eo')
        mate = me + 1 - 2 * (me % 2)
        wg, wu, wd = w_gate[0], w_up[0], w_down[0]
        n_val, wide = tok_dev * top_k, 2 * LANES
        table = jnp.concatenate([idx_loc.astype(f32).reshape(-1), gate_loc.reshape(-1)])
        n_row = -(-table.shape[0] // (wide * SUBLANES)) * SUBLANES
        table = jnp.pad(table, (0, n_row * wide - table.shape[0])).reshape(n_row, wide)
        x, table = all_gather_rows(tok_loc, table, group, 0)
        table = table.reshape(group, -1)
        ids, gates = table[:, :n_val].reshape(-1, top_k), table[:, n_val:2 * n_val].reshape(-1, top_k)

        def column(e):
            hit = ids == e.astype(f32)
            return jnp.sum(jnp.where(hit, gates, 0.0), axis=1), jnp.any(hit, axis=1).astype(f32)
        gm = jnp.stack(column(me) + column(mate), axis=1)
        a, b, h, o, dy = forward(x, gm, wg, wu, wd, dy_loc, 1)
        dg, du, u, dx, dgate, y = backward(dy, gm, a, b, o, wg, wu, wd, tok_dev, 2)
        dgate = dgate.reshape(-1, wide)
        dwg, dwu, dwd, dxs, dgate = weights(x, dg, du, h, u, dx, dgate, tok_dev, 3)
        dgate = lax.dynamic_index_in_dim(dgate.reshape(group, group, tok_dev), me, 1, keepdims=False)
        expert = jnp.arange(group, dtype=jnp.int32)[:, None, None]
        dgate = jnp.sum(jnp.where(idx_loc[None] == expert, dgate[:, :, None], 0.0), axis=0)
        return y, dxs, dgate, dwg[None], dwu[None], dwd[None]

    return jax.shard_map(device_step, mesh=mesh, in_specs=(tok_spec, tok_spec, tok_spec, exp_spec, exp_spec, exp_spec, tok_spec), out_specs=(tok_spec,) * 6, check_vma=False)
```
